32 devices in a mesh: data: 32 (over z, y, x, core).
Axes of the slice: x: 2, y: 2, z: 4, core: 2. Of those that a mesh axis runs over, the one named last changes fastest.
Arguments:
- inputs_now: bfloat16 [32768, 1536], P('data')
- targets_now: bfloat16 [32768, 4096], P('data')
- inputs_next: bfloat16 [32768, 1536], P('data')
- targets_next: bfloat16 [32768, 4096], P('data')
- w_up: float32 [1, 1536, 6144], replicated
- w_down: float32 [1, 6144, 1536], replicated
- w_head: float32 [1536, 4096], replicated
- mom_up: float32 [1, 1536, 6144], replicated
- mom_down: float32 [1, 6144, 1536], replicated
- mom_head: float32 [1536, 4096], replicated
Outputs:
- output 1: float32 [1, 1536, 6144], replicated
- output 2: float32 [1, 6144, 1536], replicated
- output 3: float32 [1536, 4096], replicated
- output 4: float32 [1, 1536, 6144], replicated
- output 5: float32 [1, 6144, 1536], replicated
- output 6: float32 [1536, 4096], replicated
- output 7: float32 [32768], P('data')
- output 8: float32 [32768, 1536], P('data')
All inputs are finite; a program needn't handle non-finite values.
Results may differ from the reference program's by a relative error of at most 0.00580266.
Values are sent between devices in bfloat16 or wider.
A program may use at most 1.75 GiB of HBM per device.

```python
import jax
import jax.numpy as jnp
from jax import lax

TOK_DEV = 1024
DATA = 32
MODEL_DIM = 1536
FF_DIM = 6144
HEAD_WIDTH = 4096
LAYERS = 1

BATCH = TOK_DEV * DATA
PROBE_ROWS = min(BATCH, 256)
MOMENTUM = 0.9
LEARN_RATE = 0.5 / LAYERS


def run_stack(w_up, w_down, hidden):
    def layer_step(hidden_in, weights):
        up_mat, down_mat = weights
        pre_act = jnp.dot(hidden_in.astype(jnp.bfloat16), up_mat.astype(jnp.bfloat16), preferred_element_type=jnp.float32)
        act_bf = jax.nn.gelu(pre_act).astype(jnp.bfloat16)
        return hidden_in + jnp.dot(act_bf, down_mat.astype(jnp.bfloat16), preferred_element_type=jnp.float32), None
    result, unused = lax.scan(layer_step, hidden, (w_up, w_down))
    return result


def head_logits(w_head, hidden):
    return jnp.dot(hidden.astype(jnp.bfloat16), w_head.astype(jnp.bfloat16), preferred_element_type=jnp.float32)


def block_loss(params, inputs, targets, loss_div):
    hidden = run_stack(params[0], params[1], inputs.astype(jnp.float32))
    logit_err = head_logits(params[2], hidden) - targets.astype(jnp.float32)
    return jnp.sum(logit_err * logit_err) / loss_div


def scaled_momentum(key, gradient, rms_axes):
    grad_rms = jnp.sqrt(jnp.mean(gradient * gradient, axis=rms_axes, keepdims=True))
    return jax.random.normal(key, gradient.shape, jnp.float32) * grad_rms


def setup_inputs(seed: int = 0) -> dict:
    key_list = jax.random.split(jax.random.key(seed), 10)
    inputs_now = jax.random.normal(key_list[0], (BATCH, MODEL_DIM), jnp.float32).astype(jnp.bfloat16)
    targets_now = jax.random.normal(key_list[1], (BATCH, HEAD_WIDTH), jnp.float32).astype(jnp.bfloat16)
    inputs_next = jax.random.normal(key_list[2], (BATCH, MODEL_DIM), jnp.float32).astype(jnp.bfloat16)
    targets_next = jax.random.normal(key_list[3], (BATCH, HEAD_WIDTH), jnp.float32).astype(jnp.bfloat16)
    w_up = jax.random.normal(key_list[4], (LAYERS, MODEL_DIM, FF_DIM), jnp.float32) * MODEL_DIM ** -0.5
    w_down = jax.random.normal(key_list[5], (LAYERS, FF_DIM, MODEL_DIM), jnp.float32) * (2.0 / (FF_DIM * LAYERS)) ** 0.5
    w_head = jax.random.normal(key_list[6], (MODEL_DIM, HEAD_WIDTH), jnp.float32) * MODEL_DIM ** -0.5
    gradients = jax.grad(block_loss)((w_up, w_down, w_head), inputs_now[:PROBE_ROWS], targets_now[:PROBE_ROWS], 2.0 * PROBE_ROWS * HEAD_WIDTH)
    return {'inputs_now': inputs_now, 'targets_now': targets_now, 'inputs_next': inputs_next, 'targets_next': targets_next, 'w_up': w_up, 'w_down': w_down, 'w_head': w_head, 'mom_up': scaled_momentum(key_list[7], gradients[0], (1, 2)), 'mom_down': scaled_momentum(key_list[8], gradients[1], (1, 2)), 'mom_head': scaled_momentum(key_list[9], gradients[2], (0, 1))}


def reference(inputs_now, targets_now, inputs_next, targets_next, w_up, w_down, w_head, mom_up, mom_down, mom_head):
    params = (w_up, w_down, w_head)
    loss_div = 2.0 * BATCH * HEAD_WIDTH

    def accumulate(running, row_block):
        block_grads = jax.grad(block_loss)(params, row_block[0], row_block[1], loss_div)
        return tuple(part_sum + part_new for part_sum, part_new in zip(running, block_grads)), None

    start_sums = tuple(jnp.zeros_like(weight) for weight in params)
    gradients, unused = lax.scan(accumulate, start_sums, (inputs_now.reshape(DATA, TOK_DEV, MODEL_DIM), targets_now.reshape(DATA, TOK_DEV, HEAD_WIDTH)))
    momenta = tuple(MOMENTUM * moment + gradient for moment, gradient in zip((mom_up, mom_down, mom_head), gradients))
    new_params = tuple(weight - LEARN_RATE * moment for weight, moment in zip(params, momenta))

    def next_block(row_block):
        hidden = run_stack(new_params[0], new_params[1], row_block[0].astype(jnp.float32))
        logit_err = head_logits(new_params[2], hidden) - row_block[1].astype(jnp.float32)
        return jnp.sum(logit_err * logit_err, axis=-1) / (2.0 * HEAD_WIDTH), hidden

    errors, hidden = lax.map(next_block, (inputs_next.reshape(DATA, TOK_DEV, MODEL_DIM), targets_next.reshape(DATA, TOK_DEV, HEAD_WIDTH)))
    return (new_params[0], new_params[1], new_params[2], momenta[0], momenta[1], momenta[2], errors.reshape(BATCH), hidden.reshape(BATCH, MODEL_DIM))
```

```python
import functools

import jax
import jax.numpy as jnp
from jax import lax
from jax.experimental import pallas as pl
from jax.experimental.pallas import tpu as pltpu
from jax.sharding import PartitionSpec as P

MOMENTUM = 0.9
RATE_BASE = 0.5
ROW_DIMS = (((0,), (0,)), ((), ()))
COL_DIMS = (((1,), (1,)), ((), ()))
MESH = pl.DeviceIdType.MESH

CORE, X, Y, Z_LOW, Z_HIGH = 1, 2, 4, 8, 16
CHUNK = 512
ACC_SLOTS, RX_SLOTS, SUM_SLOTS = 6, 4, 8
LEVELS = 4


def bit_of(me, stride):
    return lax.rem(lax.div(me, stride), 2)


def partner_of(me, stride):
    return me + stride * (1 - 2 * bit_of(me, stride))


class Part:
    def __init__(self, me, axis_chunk, order, axes, src, out, acc, rx, total, send_sem, recv_sem, load_sem, store_sem):
        self.me, self.axis_chunk, self.order = me, axis_chunk, order
        self.src, self.out, self.acc, self.rx, self.total = src, out, acc, rx, total
        self.send_sem, self.recv_sem, self.load_sem, self.store_sem = send_sem, recv_sem, load_sem, store_sem
        self.chunks = src.shape[axis_chunk] // CHUNK
        nr, nc = acc.shape[1], acc.shape[2]
        self.keep, self.send = [(0, 0, nr, nc)], [None]
        for level in range(1, LEVELS + 1):
            r0, c0, nr, nc = self.keep[-1]
            bit = bit_of(me, order[level])
            if axes[level] == 0:
                nr //= 2
                self.keep.append((pl.multiple_of(r0 + bit * nr, 16), c0, nr, nc))
                self.send.append((pl.multiple_of(r0 + (1 - bit) * nr, 16), c0, nr, nc))
            else:
                nc //= 2
                self.keep.append((r0, pl.multiple_of(c0 + bit * nc, 128), nr, nc))
                self.send.append((r0, pl.multiple_of(c0 + (1 - bit) * nc, 128), nr, nc))

    def half(self, ref, chunk, which):
        size = CHUNK // 2
        start = pl.multiple_of(chunk * CHUNK + which * size, size)
        if self.axis_chunk == 0:
            return ref.at[pl.ds(start, size), :]
        return ref.at[:, pl.ds(start, size)]

    @staticmethod
    def at(ref, slot, region):
        r0, c0, nr, nc = region
        return ref.at[slot, pl.ds(r0, nr), pl.ds(c0, nc)]

    def copy(self, phase, chunk):
        me = self.me
        acc_slot, rx_slot, sum_slot = lax.rem(chunk, ACC_SLOTS), lax.rem(chunk, RX_SLOTS), lax.rem(chunk, SUM_SLOTS)
        core = bit_of(me, CORE)
        if phase == 0:
            source, target = self.half(self.src, chunk, 1 - core), self.rx[0].at[rx_slot]
        elif phase <= LEVELS:
            source, target = self.at(self.acc, acc_slot, self.send[phase]), self.rx[phase].at[rx_slot]
        elif phase <= 2 * LEVELS:
            source = self.at(self.total, sum_slot, self.keep[2 * LEVELS + 1 - phase])
            target = source
        else:
            source, target = self.total.at[sum_slot], self.half(self.out, chunk, core)
        level = phase if phase <= LEVELS else 2 * LEVELS + 1 - phase
        return pltpu.make_async_remote_copy(
            src_ref=source,
            dst_ref=target,
            send_sem=self.send_sem.at[phase, rx_slot],
            recv_sem=self.recv_sem.at[phase, rx_slot],
            device_id=(partner_of(me, self.order[level]),),
            device_id_type=MESH,
        )

    def load(self, chunk):
        slot = lax.rem(chunk, ACC_SLOTS)
        return pltpu.make_async_copy(self.half(self.src, chunk, bit_of(self.me, CORE)), self.acc.at[slot], self.load_sem.at[slot])

    def store(self, chunk):
        slot = lax.rem(chunk, SUM_SLOTS)
        return pltpu.make_async_copy(self.total.at[slot], self.half(self.out, chunk, bit_of(self.me, CORE)), self.store_sem.at[slot])

    def add(self, chunk, level, region, parent, target, target_slot):
        acc_slot, rx_slot = lax.rem(chunk, ACC_SLOTS), lax.rem(chunk, RX_SLOTS)
        r0, c0, nr, nc = region
        rel_r, rel_c = r0 - parent[0], c0 - parent[1]
        rows = max(16, min(nr, 24576 // nc))
        rx = self.rx[level]

        def body(i, carry):
            at_r = pl.multiple_of(r0 + i * rows, 16)
            from_r = pl.multiple_of(rel_r + i * rows, 16)
            to_c = c0 if isinstance(c0, int) else pl.multiple_of(c0, 128)
            from_c = rel_c if isinstance(rel_c, int) else pl.multiple_of(rel_c, 128)
            mine = self.acc[acc_slot, pl.ds(at_r, rows), pl.ds(to_c, nc)].astype(jnp.float32)
            theirs = rx[rx_slot, pl.ds(from_r, rows), pl.ds(from_c, nc)].astype(jnp.float32)
            target[target_slot, pl.ds(at_r, rows), pl.ds(to_c, nc)] = (mine + theirs).astype(jnp.bfloat16)
            return carry

        lax.fori_loop(0, nr // rows, body, 0)

    def stage(self, number, chunk):
        if number == 0:
            self.load(chunk).start()
            self.copy(0, chunk).start()
            return
        if number == 1:
            self.load(chunk).wait()
        self.copy(number - 1, chunk).wait()
        if number <= LEVELS:
            slot = lax.rem(chunk, ACC_SLOTS)
            parent = self.keep[number - 1]
            self.add(chunk, number - 1, self.send[number], parent, self.acc, slot)
            self.copy(number, chunk).start()
            self.add(chunk, number - 1, self.keep[number], parent, self.acc, slot)
        elif number == LEVELS + 1:
            last = self.keep[LEVELS]
            self.add(chunk, LEVELS, last, last, self.total, lax.rem(chunk, SUM_SLOTS))
            self.copy(number, chunk).start()
        elif number <= 2 * LEVELS:
            self.copy(number, chunk).start()
        elif number == 2 * LEVELS + 1:
            self.copy(number, chunk).start()
            self.store(chunk).start()
        else:
            self.store(chunk).wait()


PART_REFS = 2 + LEVELS + 1 + 4


def sum_kernel(up_ref, down_ref, up_out, down_out, *scratch):
    me = lax.axis_index('data')
    strides = (CORE, X, Y, Z_LOW, Z_HIGH)
    barrier = pltpu.get_barrier_semaphore()
    for stride in strides:
        pl.semaphore_signal(barrier, inc=1, device_id=(partner_of(me, stride),), device_id_type=MESH)
    pl.semaphore_wait(barrier, len(strides))

    def build(axis_chunk, order, axes, src, out, refs):
        acc, rx, total = refs[0], refs[1:2 + LEVELS], refs[2 + LEVELS]
        return Part(me, axis_chunk, order, axes, src, out, acc, rx, total, *refs[3 + LEVELS:])

    parts = (
        build(1, (CORE, X, Z_LOW, Y, Z_HIGH), (1, 1, 0, 0, 0), up_ref, up_out, scratch[:PART_REFS]),
        build(0, (CORE, Y, Z_LOW, X, Z_HIGH), (0, 0, 0, 0, 0), down_ref, down_out, scratch[PART_REFS:]),
    )
    stages = 2 * LEVELS + 3

    def tick(t, carry):
        for number in range(stages):
            for part in parts:
                chunk = t - number

                @pl.when(jnp.logical_and(chunk >= 0, chunk < part.chunks))
                def _():
                    part.stage(number, chunk)
        return carry

    lax.fori_loop(0, max(part.chunks for part in parts) + stages - 1, tick, 0)


def part_scratch(rows, cols, axes):
    shapes = [pltpu.VMEM((ACC_SLOTS, rows, cols), jnp.bfloat16), pltpu.VMEM((RX_SLOTS, rows, cols), jnp.bfloat16)]
    nr, nc = rows, cols
    for level in range(1, LEVELS + 1):
        nr, nc = (nr // 2, nc) if axes[level] == 0 else (nr, nc // 2)
        shapes.append(pltpu.VMEM((RX_SLOTS, nr, nc), jnp.bfloat16))
    shapes.append(pltpu.VMEM((SUM_SLOTS, rows, cols), jnp.bfloat16))
    phases = 2 * LEVELS + 2
    shapes += [pltpu.SemaphoreType.DMA((phases, RX_SLOTS)), pltpu.SemaphoreType.DMA((phases, RX_SLOTS))]
    shapes += [pltpu.SemaphoreType.DMA((ACC_SLOTS,)), pltpu.SemaphoreType.DMA((SUM_SLOTS,))]
    return shapes


def sum_gradients(up_local, down_local):
    scratch = part_scratch(up_local.shape[0], CHUNK // 2, (1, 1, 0, 0, 0))
    scratch += part_scratch(CHUNK // 2, down_local.shape[1], (0, 0, 0, 0, 0))
    any_spec = pl.BlockSpec(memory_space=pl.ANY)
    size = up_local.size + down_local.size
    return pl.pallas_call(
        sum_kernel,
        out_shape=[jax.ShapeDtypeStruct(up_local.shape, jnp.bfloat16), jax.ShapeDtypeStruct(down_local.shape, jnp.bfloat16)],
        in_specs=[any_spec] * 2,
        out_specs=[any_spec] * 2,
        scratch_shapes=scratch,
        compiler_params=pltpu.CompilerParams(collective_id=0, has_side_effects=True, vmem_limit_bytes=60 * 2**20),
        cost_estimate=pl.CostEstimate(flops=280 * 10**9, bytes_accessed=8 * size, transcendentals=0),
        name='sum_gradients',
    )(up_local, down_local)


def update(weight_ref, moment_ref, grad_ref, weight_out, moment_out, rate):
    new_moment = MOMENTUM * moment_ref[...] + grad_ref[...].astype(jnp.float32)
    new_weight = weight_ref[...] - rate * new_moment
    moment_out[...] = new_moment
    weight_out[...] = new_weight
    return new_weight.astype(jnp.bfloat16)


def up_kernel(rate, rows_ref, weight_ref, moment_ref, grad_ref, weight_out, moment_out, act_out):
    weight_bf = update(weight_ref, moment_ref, grad_ref, weight_out, moment_out, rate)
    pre_act = jnp.dot(rows_ref[...], weight_bf, preferred_element_type=jnp.float32)
    act_out[...] = jax.nn.gelu(pre_act).astype(jnp.bfloat16)


def down_kernel(rate, rows_ref, act_ref, weight_ref, moment_ref, grad_ref, weight_out, moment_out, hidden_out, hidden_bf_out):
    step = pl.program_id(0)
    weight_bf = update(weight_ref, moment_ref, grad_ref, weight_out, moment_out, rate)

    @pl.when(step == 0)
    def _():
        hidden_out[...] = rows_ref[...].astype(jnp.float32)

    hidden_out[...] += jnp.dot(act_ref[...], weight_bf, preferred_element_type=jnp.float32)

    @pl.when(step == pl.num_programs(0) - 1)
    def _():
        hidden_bf_out[...] = hidden_out[...].astype(jnp.bfloat16)


def head_kernel(rate, hidden_ref, target_ref, weight_ref, moment_ref, grad_ref, weight_out, moment_out, error_out):
    weight_bf = update(weight_ref, moment_ref, grad_ref, weight_out, moment_out, rate)
    logits = jnp.dot(hidden_ref[...], weight_bf, preferred_element_type=jnp.float32)
    logit_err = logits - target_ref[...].astype(jnp.float32)
    squares = logit_err * logit_err
    folded = squares[:, :128]
    for start in range(128, squares.shape[1], 128):
        folded += squares[:, start:start + 128]

    @pl.when(pl.program_id(0) == 0)
    def _():
        error_out[...] = jnp.zeros_like(error_out)

    error_out[...] += folded


def whole(shape):
    return pl.BlockSpec(shape, lambda i: (0, 0))


def step_call(kernel, rate, steps, in_specs, out_specs, out_shape, flops, name, args):
    return pl.pallas_call(
        functools.partial(kernel, rate),
        grid=(steps,),
        in_specs=in_specs,
        out_specs=out_specs,
        out_shape=out_shape,
        compiler_params=pltpu.CompilerParams(dimension_semantics=('arbitrary',), vmem_limit_bytes=60 * 2**20),
        cost_estimate=pl.CostEstimate(flops=flops, bytes_accessed=16 * args[-1].size, transcendentals=0),
        name=name,
    )(*args)


def second_up(rows, weight, moment, grad, rate, tile=256):
    tokens, (model, width) = rows.shape[0], weight.shape
    cols = pl.BlockSpec((model, tile), lambda i: (0, i))
    return step_call(
        up_kernel, rate, width // tile,
        [whole(rows.shape), cols, cols, cols],
        [cols, cols, pl.BlockSpec((tokens, tile), lambda i: (0, i))],
        [jax.ShapeDtypeStruct(weight.shape, jnp.float32)] * 2 + [jax.ShapeDtypeStruct((tokens, width), jnp.bfloat16)],
        2 * tokens * model * width, 'second_up', (rows, weight, moment, grad))


def second_down(rows, act, weight, moment, grad, rate, tile=256):
    tokens, (width, model) = rows.shape[0], weight.shape
    band = pl.BlockSpec((tile, model), lambda i: (i, 0))
    return step_call(
        down_kernel, rate, width // tile,
        [whole(rows.shape), pl.BlockSpec((tokens, tile), lambda i: (0, i)), band, band, band],
        [band, band, whole(rows.shape), whole(rows.shape)],
        [jax.ShapeDtypeStruct(weight.shape, jnp.float32)] * 2 + [jax.ShapeDtypeStruct(rows.shape, jnp.float32), jax.ShapeDtypeStruct(rows.shape, jnp.bfloat16)],
        2 * tokens * model * width, 'second_down', (rows, act, weight, moment, grad))


def second_head(hidden_bf, targets, weight, moment, grad, rate, tile=256):
    tokens, (model, width) = hidden_bf.shape[0], weight.shape
    cols = pl.BlockSpec((model, tile), lambda i: (0, i))
    return step_call(
        head_kernel, rate, width // tile,
        [whole(hidden_bf.shape), pl.BlockSpec((tokens, tile), lambda i: (0, i)), cols, cols, cols],
        [cols, cols, whole((tokens, 128))],
        [jax.ShapeDtypeStruct(weight.shape, jnp.float32)] * 2 + [jax.ShapeDtypeStruct((tokens, 128), jnp.float32)],
        2 * tokens * model * width, 'second_head', (hidden_bf, targets, weight, moment, grad))


def solution(mesh):
    data_size = mesh.shape['data']

    def device_step(inputs_now, targets_now, inputs_next, targets_next, w_up, w_down, w_head, mom_up, mom_down, mom_head):
        rate = RATE_BASE / w_up.shape[0]
        loss_scale = 1.0 / (inputs_now.shape[0] * data_size * w_head.shape[1])
        up, down, up_moment, down_moment = w_up[0], w_down[0], mom_up[0], mom_down[0]
        up_bf, down_bf, head_bf = up.astype(jnp.bfloat16), down.astype(jnp.bfloat16), w_head.astype(jnp.bfloat16)

        pre_act = jnp.dot(inputs_now, up_bf, preferred_element_type=jnp.float32)
        act_f32, gelu_back = jax.vjp(jax.nn.gelu, pre_act)
        act_bf = act_f32.astype(jnp.bfloat16)
        hidden = inputs_now.astype(jnp.float32) + jnp.dot(act_bf, down_bf, preferred_element_type=jnp.float32)
        top_bf = hidden.astype(jnp.bfloat16)
        logits = jnp.dot(top_bf, head_bf, preferred_element_type=jnp.float32)
        grad_logits = ((logits - targets_now.astype(jnp.float32)) * loss_scale).astype(jnp.bfloat16)

        head_local = lax.dot_general(top_bf, grad_logits, ROW_DIMS, preferred_element_type=jnp.float32).astype(jnp.bfloat16)
        grad_head = lax.psum(head_local, 'data')
        grad_hidden = lax.dot_general(grad_logits, head_bf, COL_DIMS, preferred_element_type=jnp.float32)
        grad_hidden_bf = grad_hidden.astype(jnp.bfloat16)
        down_local = lax.dot_general(act_bf, grad_hidden_bf, ROW_DIMS, preferred_element_type=jnp.float32).astype(jnp.bfloat16)
        grad_act = lax.dot_general(grad_hidden_bf, down_bf, COL_DIMS, preferred_element_type=jnp.float32)
        grad_pre = gelu_back(grad_act)[0].astype(jnp.bfloat16)
        up_local = lax.dot_general(inputs_now, grad_pre, ROW_DIMS, preferred_element_type=jnp.float32).astype(jnp.bfloat16)
        grad_up, grad_down = sum_gradients(up_local, down_local)

        up_new, up_moment_new, act_next = second_up(inputs_next, up, up_moment, grad_up, rate)
        down_new, down_moment_new, hidden_next, hidden_next_bf = second_down(inputs_next, act_next, down, down_moment, grad_down, rate)
        head_new, head_moment_new, squares = second_head(hidden_next_bf, targets_next, w_head, mom_head, grad_head, rate)
        errors = jnp.sum(squares, axis=-1) / (2.0 * w_head.shape[1])
        return (up_new[None], down_new[None], head_new, up_moment_new[None], down_moment_new[None], head_moment_new, errors, hidden_next)

    row_spec = P('data', None)
    whole3, whole2 = P(None, None, None), P(None, None)
    in_specs = (row_spec, row_spec, row_spec, row_spec, whole3, whole3, whole2, whole3, whole3, whole2)
    out_specs = (whole3, whole3, whole2, whole3, whole3, whole2, P('data'), row_spec)
    return jax.shard_map(device_step, mesh=mesh, in_specs=in_specs, out_specs=out_specs, check_vma=False)
```

```python
import functools

import jax
import jax.numpy as jnp
from jax import lax
from jax.experimental import pallas as pl
from jax.experimental.pallas import tpu as pltpu
from jax.sharding import PartitionSpec as P

MOMENTUM = 0.9
RATE_BASE = 0.5
ROW_DIMS = (((0,), (0,)), ((), ()))
COL_DIMS = (((1,), (1,)), ((), ()))
MESH = pl.DeviceIdType.MESH

CORE, X, Y, Z_LOW, Z_HIGH = 1, 2, 4, 8, 16
CHUNK = 512
ACC_SLOTS, RX_SLOTS, SUM_SLOTS = 6, 4, 8
LEVELS = 4


def bit_of(me, stride):
    return lax.rem(lax.div(me, stride), 2)


def partner_of(me, stride):
    return me + stride * (1 - 2 * bit_of(me, stride))


class Part:
    def __init__(self, me, axis_chunk, order, axes, src, out, acc, rx, total, send_sem, recv_sem, load_sem, store_sem):
        self.me, self.axis_chunk, self.order = me, axis_chunk, order
        self.src, self.out, self.acc, self.rx, self.total = src, out, acc, rx, total
        self.send_sem, self.recv_sem, self.load_sem, self.store_sem = send_sem, recv_sem, load_sem, store_sem
        self.chunks = src.shape[axis_chunk] // CHUNK
        nr, nc = acc.shape[1], acc.shape[2]
        self.keep, self.send = [(0, 0, nr, nc)], [None]
        for level in range(1, LEVELS + 1):
            r0, c0, nr, nc = self.keep[-1]
            bit = bit_of(me, order[level])
            if axes[level] == 0:
                nr //= 2
                self.keep.append((pl.multiple_of(r0 + bit * nr, 16), c0, nr, nc))
                self.send.append((pl.multiple_of(r0 + (1 - bit) * nr, 16), c0, nr, nc))
            else:
                nc //= 2
                self.keep.append((r0, pl.multiple_of(c0 + bit * nc, 128), nr, nc))
                self.send.append((r0, pl.multiple_of(c0 + (1 - bit) * nc, 128), nr, nc))

    def half(self, ref, chunk, which):
        size = CHUNK // 2
        start = pl.multiple_of(chunk * CHUNK + which * size, size)
        if self.axis_chunk == 0:
            return ref.at[pl.ds(start, size), :]
        return ref.at[:, pl.ds(start, size)]

    @staticmethod
    def at(ref, slot, region):
        r0, c0, nr, nc = region
        return ref.at[slot, pl.ds(r0, nr), pl.ds(c0, nc)]

    def copy(self, phase, chunk):
        me = self.me
        acc_slot, rx_slot, sum_slot = lax.rem(chunk, ACC_SLOTS), lax.rem(chunk, RX_SLOTS), lax.rem(chunk, SUM_SLOTS)
        core = bit_of(me, CORE)
        if phase == 0:
            source, target = self.half(self.src, chunk, 1 - core), self.rx[0].at[rx_slot]
        elif phase <= LEVELS:
            source, target = self.at(self.acc, acc_slot, self.send[phase]), self.rx[phase].at[rx_slot]
        elif phase <= 2 * LEVELS:
            source = self.at(self.total, sum_slot, self.keep[2 * LEVELS + 1 - phase])
            target = source
        else:
            source, target = self.total.at[sum_slot], self.half(self.out, chunk, core)
        level = phase if phase <= LEVELS else 2 * LEVELS + 1 - phase
        return pltpu.make_async_remote_copy(
            src_ref=source,
            dst_ref=target,
            send_sem=self.send_sem.at[phase, rx_slot],
            recv_sem=self.recv_sem.at[phase, rx_slot],
            device_id=(partner_of(me, self.order[level]),),
            device_id_type=MESH,
        )

    def load(self, chunk):
        slot = lax.rem(chunk, ACC_SLOTS)
        return pltpu.make_async_copy(self.half(self.src, chunk, bit_of(self.me, CORE)), self.acc.at[slot], self.load_sem.at[slot])

    def store(self, chunk):
        slot = lax.rem(chunk, SUM_SLOTS)
        return pltpu.make_async_copy(self.total.at[slot], self.half(self.out, chunk, bit_of(self.me, CORE)), self.store_sem.at[slot])

    def add(self, chunk, level, region, parent, target, target_slot):
        acc_slot, rx_slot = lax.rem(chunk, ACC_SLOTS), lax.rem(chunk, RX_SLOTS)
        r0, c0, nr, nc = region
        rel_r, rel_c = r0 - parent[0], c0 - parent[1]
        rows = max(16, min(nr, 24576 // nc))
        rx = self.rx[level]

        def body(i, carry):
            at_r = pl.multiple_of(r0 + i * rows, 16)
            from_r = pl.multiple_of(rel_r + i * rows, 16)
            to_c = c0 if isinstance(c0, int) else pl.multiple_of(c0, 128)
            from_c = rel_c if isinstance(rel_c, int) else pl.multiple_of(rel_c, 128)
            mine = self.acc[acc_slot, pl.ds(at_r, rows), pl.ds(to_c, nc)].astype(jnp.float32)
            theirs = rx[rx_slot, pl.ds(from_r, rows), pl.ds(from_c, nc)].astype(jnp.float32)
            target[target_slot, pl.ds(at_r, rows), pl.ds(to_c, nc)] = (mine + theirs).astype(jnp.bfloat16)
            return carry

        lax.fori_loop(0, nr // rows, body, 0)

    def stage(self, number, chunk):
        if number == 0:
            self.load(chunk).start()
            self.copy(0, chunk).start()
            return
        if number == 1:
            self.load(chunk).wait()
        self.copy(number - 1, chunk).wait()
        if number <= LEVELS:
            slot = lax.rem(chunk, ACC_SLOTS)
            parent = self.keep[number - 1]
            self.add(chunk, number - 1, self.send[number], parent, self.acc, slot)
            self.copy(number, chunk).start()
            self.add(chunk, number - 1, self.keep[number], parent, self.acc, slot)
        elif number == LEVELS + 1:
            last = self.keep[LEVELS]
            self.add(chunk, LEVELS, last, last, self.total, lax.rem(chunk, SUM_SLOTS))
            self.copy(number, chunk).start()
        elif number <= 2 * LEVELS:
            self.copy(number, chunk).start()
        elif number == 2 * LEVELS + 1:
            self.copy(number, chunk).start()
            self.store(chunk).start()
        else:
            self.store(chunk).wait()


PART_REFS = 2 + LEVELS + 1 + 4


def sum_kernel(up_ref, down_ref, later_ref, earlier_ref, up_out, down_out, later_out, *scratch):
    me = lax.axis_index('data')
    strides = (CORE, X, Y, Z_LOW, Z_HIGH)
    barrier = pltpu.get_barrier_semaphore()
    for stride in strides:
        pl.semaphore_signal(barrier, inc=1, device_id=(partner_of(me, stride),), device_id_type=MESH)
    pl.semaphore_wait(barrier, len(strides))

    def build(axis_chunk, order, axes, src, out, refs):
        acc, rx, total = refs[0], refs[1:2 + LEVELS], refs[2 + LEVELS]
        return Part(me, axis_chunk, order, axes, src, out, acc, rx, total, *refs[3 + LEVELS:])

    parts = (
        build(1, (CORE, X, Z_LOW, Y, Z_HIGH), (1, 1, 0, 0, 0), up_ref, up_out, scratch[:PART_REFS]),
        build(0, (CORE, Y, Z_LOW, X, Z_HIGH), (0, 0, 0, 0, 0), down_ref, down_out, scratch[PART_REFS:]),
    )
    stages = 2 * LEVELS + 3

    def tick(t, carry):
        for number in range(stages):
            for part in parts:
                chunk = t - number

                @pl.when(jnp.logical_and(chunk >= 0, chunk < part.chunks))
                def _():
                    part.stage(number, chunk)
        return carry

    lax.fori_loop(0, max(part.chunks for part in parts) + stages - 1, tick, 0)


def part_scratch(rows, cols, axes):
    shapes = [pltpu.VMEM((ACC_SLOTS, rows, cols), jnp.bfloat16), pltpu.VMEM((RX_SLOTS, rows, cols), jnp.bfloat16)]
    nr, nc = rows, cols
    for level in range(1, LEVELS + 1):
        nr, nc = (nr // 2, nc) if axes[level] == 0 else (nr, nc // 2)
        shapes.append(pltpu.VMEM((RX_SLOTS, nr, nc), jnp.bfloat16))
    shapes.append(pltpu.VMEM((SUM_SLOTS, rows, cols), jnp.bfloat16))
    phases = 2 * LEVELS + 2
    shapes += [pltpu.SemaphoreType.DMA((phases, RX_SLOTS)), pltpu.SemaphoreType.DMA((phases, RX_SLOTS))]
    shapes += [pltpu.SemaphoreType.DMA((ACC_SLOTS,)), pltpu.SemaphoreType.DMA((SUM_SLOTS,))]
    return shapes


def sum_gradients(up_local, down_local, later, earlier):
    scratch = part_scratch(up_local.shape[0], CHUNK // 2, (1, 1, 0, 0, 0))
    scratch += part_scratch(CHUNK // 2, down_local.shape[1], (0, 0, 0, 0, 0))
    any_spec = pl.BlockSpec(memory_space=pl.ANY)
    size = up_local.size + down_local.size
    return pl.pallas_call(
        sum_kernel,
        out_shape=[jax.ShapeDtypeStruct(array.shape, jnp.bfloat16) for array in (up_local, down_local, later)],
        in_specs=[any_spec] * 4,
        out_specs=[any_spec] * 3,
        input_output_aliases={2: 2},
        scratch_shapes=scratch,
        compiler_params=pltpu.CompilerParams(collective_id=0, has_side_effects=True, vmem_limit_bytes=60 * 2**20),
        cost_estimate=pl.CostEstimate(flops=280 * 10**9, bytes_accessed=8 * size, transcendentals=0),
        name='sum_gradients',
    )(up_local, down_local, later, earlier)


def first_up_kernel(rows_ref, weight_ref, pre_out, act_out):
    pre_act = jnp.dot(rows_ref[...], weight_ref[...].astype(jnp.bfloat16), preferred_element_type=jnp.float32)
    pre_out[...] = pre_act
    act_out[...] = jax.nn.gelu(pre_act).astype(jnp.bfloat16)


def first_down_kernel(rows_ref, act_ref, weight_ref, top_out, hidden):
    step = pl.program_id(0)

    @pl.when(step == 0)
    def _():
        hidden[...] = rows_ref[...].astype(jnp.float32)

    hidden[...] += jnp.dot(act_ref[...], weight_ref[...].astype(jnp.bfloat16), preferred_element_type=jnp.float32)

    @pl.when(step == pl.num_programs(0) - 1)
    def _():
        top_out[...] = hidden[...].astype(jnp.bfloat16)


def first_head_kernel(loss_scale, top_ref, target_ref, weight_ref, low_out, high_out, cotangent_out, cotangent):
    step = pl.program_id(0)

    @pl.when(step == 0)
    def _():
        cotangent[...] = jnp.zeros_like(cotangent)

    weight_bf = weight_ref[...].astype(jnp.bfloat16)
    logits = jnp.dot(top_ref[...], weight_bf, preferred_element_type=jnp.float32)
    grad_logits = ((logits - target_ref[...].astype(jnp.float32)) * loss_scale).astype(jnp.bfloat16)
    cotangent[...] += lax.dot_general(grad_logits, weight_bf, COL_DIMS, preferred_element_type=jnp.float32)
    share = lax.dot_general(top_ref[...], grad_logits, ROW_DIMS, preferred_element_type=jnp.float32).astype(jnp.bfloat16)
    low = low_out.shape[0]
    low_out[...] = share[:low]
    high_out[...] = share[low:]

    @pl.when(step == pl.num_programs(0) - 1)
    def _():
        cotangent_out[...] = cotangent[...].astype(jnp.bfloat16)


def update(weight_ref, moment_ref, grad, weight_out, moment_out, rate):
    new_moment = MOMENTUM * moment_ref[...] + grad.astype(jnp.float32)
    new_weight = weight_ref[...] - rate * new_moment
    moment_out[...] = new_moment
    weight_out[...] = new_weight
    return new_weight.astype(jnp.bfloat16)


def up_kernel(rate, rows_ref, weight_ref, moment_ref, grad_ref, weight_out, moment_out, act_out):
    weight_bf = update(weight_ref, moment_ref, grad_ref[...], weight_out, moment_out, rate)
    pre_act = jnp.dot(rows_ref[...], weight_bf, preferred_element_type=jnp.float32)
    act_out[...] = jax.nn.gelu(pre_act).astype(jnp.bfloat16)


def down_kernel(rate, rows_ref, act_ref, weight_ref, moment_ref, grad_ref, weight_out, moment_out, hidden_out, hidden_bf_out):
    step = pl.program_id(0)
    weight_bf = update(weight_ref, moment_ref, grad_ref[...], weight_out, moment_out, rate)

    @pl.when(step == 0)
    def _():
        hidden_out[...] = rows_ref[...].astype(jnp.float32)

    hidden_out[...] += jnp.dot(act_ref[...], weight_bf, preferred_element_type=jnp.float32)

    @pl.when(step == pl.num_programs(0) - 1)
    def _():
        hidden_bf_out[...] = hidden_out[...].astype(jnp.bfloat16)


def head_kernel(rate, hidden_ref, target_ref, weight_ref, moment_ref, low_ref, high_ref, weight_out, moment_out, error_out):
    grad = jnp.concatenate([low_ref[...], high_ref[...]], axis=0)
    weight_bf = update(weight_ref, moment_ref, grad, weight_out, moment_out, rate)
    logits = jnp.dot(hidden_ref[...], weight_bf, preferred_element_type=jnp.float32)
    logit_err = logits - target_ref[...].astype(jnp.float32)
    squares = logit_err * logit_err
    folded = squares[:, :128]
    for start in range(128, squares.shape[1], 128):
        folded += squares[:, start:start + 128]

    @pl.when(pl.program_id(0) == 0)
    def _():
        error_out[...] = jnp.zeros_like(error_out)

    error_out[...] += folded


def whole(shape):
    return pl.BlockSpec(shape, lambda i: (0, 0))


def step_call(kernel, rate, steps, in_specs, out_specs, out_shape, flops, name, args):
    return pl.pallas_call(
        functools.partial(kernel, rate),
        grid=(steps,),
        in_specs=in_specs,
        out_specs=out_specs,
        out_shape=out_shape,
        compiler_params=pltpu.CompilerParams(dimension_semantics=('arbitrary',), vmem_limit_bytes=60 * 2**20),
        cost_estimate=pl.CostEstimate(flops=flops, bytes_accessed=16 * args[-1].size, transcendentals=0),
        name=name,
    )(*args)


def low_rows(model):
    return model * 5 // 12 // 16 * 16


def first_call(kernel, steps, in_specs, out_specs, out_shape, scratch, flops, name, args):
    return pl.pallas_call(
        kernel,
        grid=(steps,),
        in_specs=in_specs,
        out_specs=out_specs,
        out_shape=out_shape,
        scratch_shapes=scratch,
        compiler_params=pltpu.CompilerParams(dimension_semantics=('arbitrary',), vmem_limit_bytes=60 * 2**20),
        cost_estimate=pl.CostEstimate(flops=flops, bytes_accessed=4 * args[-1].size, transcendentals=0),
        name=name,
    )(*args)


def first_up(rows, weight, tile=512):
    tokens, (model, width) = rows.shape[0], weight.shape
    cols = pl.BlockSpec((tokens, tile), lambda i: (0, i))
    return first_call(
        first_up_kernel, width // tile, [whole(rows.shape), pl.BlockSpec((model, tile), lambda i: (0, i))], [cols, cols],
        [jax.ShapeDtypeStruct((tokens, width), jnp.float32), jax.ShapeDtypeStruct((tokens, width), jnp.bfloat16)],
        [], 2 * tokens * model * width, 'first_up', (rows, weight))


def first_down(rows, act, weight, tile=512):
    tokens, (width, model) = rows.shape[0], weight.shape
    return first_call(
        first_down_kernel, width // tile,
        [whole(rows.shape), pl.BlockSpec((tokens, tile), lambda i: (0, i)), pl.BlockSpec((tile, model), lambda i: (i, 0))],
        whole(rows.shape), jax.ShapeDtypeStruct(rows.shape, jnp.bfloat16),
        [pltpu.VMEM(rows.shape, jnp.float32)], 2 * tokens * model * width, 'first_down', (rows, act, weight))


def first_head(top_bf, targets, weight, loss_scale, tile=512):
    tokens, (model, width) = top_bf.shape[0], weight.shape
    low = low_rows(model)
    shares = [pl.BlockSpec((rows, tile), lambda i: (0, i)) for rows in (low, model - low)]
    share_shapes = [jax.ShapeDtypeStruct((rows, width), jnp.bfloat16) for rows in (low, model - low)]
    return first_call(
        functools.partial(first_head_kernel, loss_scale), width // tile,
        [whole(top_bf.shape), pl.BlockSpec((tokens, tile), lambda i: (0, i)), pl.BlockSpec((model, tile), lambda i: (0, i))],
        [*shares, whole(top_bf.shape)], [*share_shapes, jax.ShapeDtypeStruct(top_bf.shape, jnp.bfloat16)],
        [pltpu.VMEM(top_bf.shape, jnp.float32)], 6 * tokens * model * width, 'first_head', (top_bf, targets, weight))


def second_up(rows, weight, moment, grad, rate, tile=256):
    tokens, (model, width) = rows.shape[0], weight.shape
    cols = pl.BlockSpec((model, tile), lambda i: (0, i))
    return step_call(
        up_kernel, rate, width // tile,
        [whole(rows.shape), cols, cols, cols],
        [cols, cols, pl.BlockSpec((tokens, tile), lambda i: (0, i))],
        [jax.ShapeDtypeStruct(weight.shape, jnp.float32)] * 2 + [jax.ShapeDtypeStruct((tokens, width), jnp.bfloat16)],
        2 * tokens * model * width, 'second_up', (rows, weight, moment, grad))


def second_down(rows, act, weight, moment, grad, rate, tile=384):
    tokens, (width, model) = rows.shape[0], weight.shape
    band = pl.BlockSpec((tile, model), lambda i: (i, 0))
    return step_call(
        down_kernel, rate, width // tile,
        [whole(rows.shape), pl.BlockSpec((tokens, tile), lambda i: (0, i)), band, band, band],
        [band, band, whole(rows.shape), whole(rows.shape)],
        [jax.ShapeDtypeStruct(weight.shape, jnp.float32)] * 2 + [jax.ShapeDtypeStruct(rows.shape, jnp.float32), jax.ShapeDtypeStruct(rows.shape, jnp.bfloat16)],
        2 * tokens * model * width, 'second_down', (rows, act, weight, moment, grad))


def second_head(hidden_bf, targets, weight, moment, low, high, rate, tile=256):
    tokens, (model, width) = hidden_bf.shape[0], weight.shape
    cols = pl.BlockSpec((model, tile), lambda i: (0, i))
    shares = [pl.BlockSpec((low.shape[0], tile), lambda i: (0, i)), pl.BlockSpec((high.shape[0], tile), lambda i: (0, i))]
    return step_call(
        head_kernel, rate, width // tile,
        [whole(hidden_bf.shape), pl.BlockSpec((tokens, tile), lambda i: (0, i)), cols, cols, *shares],
        [cols, cols, whole((tokens, 128))],
        [jax.ShapeDtypeStruct(weight.shape, jnp.float32)] * 2 + [jax.ShapeDtypeStruct((tokens, 128), jnp.float32)],
        2 * tokens * model * width, 'second_head', (hidden_bf, targets, weight, moment, low, high))


def solution(mesh):
    data_size = mesh.shape['data']

    def device_step(inputs_now, targets_now, inputs_next, targets_next, w_up, w_down, w_head, mom_up, mom_down, mom_head):
        rate = RATE_BASE / w_up.shape[0]
        loss_scale = 1.0 / (inputs_now.shape[0] * data_size * w_head.shape[1])
        up, down, up_moment, down_moment = w_up[0], w_down[0], mom_up[0], mom_down[0]
        down_bf = down.astype(jnp.bfloat16)

        pre_act, act_bf = first_up(inputs_now, up)
        top_bf = first_down(inputs_now, act_bf, down)
        low_local, high_local, grad_hidden_bf = first_head(top_bf, targets_now, w_head, loss_scale)
        grad_low = lax.psum(low_local, 'data')
        down_local = lax.dot_general(act_bf, grad_hidden_bf, ROW_DIMS, preferred_element_type=jnp.float32).astype(jnp.bfloat16)
        grad_act = lax.dot_general(grad_hidden_bf, down_bf, COL_DIMS, preferred_element_type=jnp.float32)
        gelu_back = jax.vjp(jax.nn.gelu, pre_act)[1]
        grad_pre = gelu_back(grad_act)[0].astype(jnp.bfloat16)
        up_local = lax.dot_general(inputs_now, grad_pre, ROW_DIMS, preferred_element_type=jnp.float32).astype(jnp.bfloat16)
        grad_up, grad_down, high_local = sum_gradients(up_local, down_local, high_local, grad_low)
        grad_high = lax.psum(high_local, 'data')

        up_new, up_moment_new, act_next = second_up(inputs_next, up, up_moment, grad_up, rate)
        down_new, down_moment_new, hidden_next, hidden_next_bf = second_down(inputs_next, act_next, down, down_moment, grad_down, rate)
        head_new, head_moment_new, squares = second_head(hidden_next_bf, targets_next, w_head, mom_head, grad_low, grad_high, rate)
        errors = jnp.sum(squares, axis=-1) / (2.0 * w_head.shape[1])
        return (up_new[None], down_new[None], head_new, up_moment_new[None], down_moment_new[None], head_moment_new, errors, hidden_next)

    row_spec = P('data', None)
    whole3, whole2 = P(None, None, None), P(None, None)
    in_specs = (row_spec, row_spec, row_spec, row_spec, whole3, whole3, whole2, whole3, whole3, whole2)
    out_specs = (whole3, whole3, whole2, whole3, whole3, whole2, P('data'), row_spec)
    return jax.shard_map(device_step, mesh=mesh, in_specs=in_specs, out_specs=out_specs, check_vma=False)
```

```python
import functools

import jax
import jax.numpy as jnp
from jax import lax
from jax.experimental import pallas as pl
from jax.experimental.pallas import tpu as pltpu
from jax.sharding import PartitionSpec as P

MOMENTUM = 0.9
RATE_BASE = 0.5
ROW_DIMS = (((0,), (0,)), ((), ()))
COL_DIMS = (((1,), (1,)), ((), ()))
MESH = pl.DeviceIdType.MESH

CORE, X, Y, Z_LOW, Z_HIGH = 1, 2, 4, 8, 16
CHUNK = 256
ACC_SLOTS, RX_SLOTS, SUM_SLOTS = 6, 4, 8
LEVELS = 4


def bit_of(me, stride):
    return lax.rem(lax.div(me, stride), 2)


def partner_of(me, stride):
    return me + stride * (1 - 2 * bit_of(me, stride))


class Part:
    def __init__(self, me, axis_chunk, order, axes, src, out, span, first, acc, rx, total, send_sem, recv_sem, load_sem, store_sem):
        self.me, self.axis_chunk, self.order = me, axis_chunk, order
        self.src, self.out, self.acc, self.rx, self.total = src, out, acc, rx, total
        self.send_sem, self.recv_sem, self.load_sem, self.store_sem = send_sem, recv_sem, load_sem, store_sem
        self.base, self.chunks = span
        self.first = first
        self.acc_slots, self.rx_slots, self.sum_slots = acc.shape[0], rx[0].shape[0], total.shape[0]
        nr, nc = acc.shape[1], acc.shape[2]
        self.keep, self.send = [(0, 0, nr, nc)], [None]
        for level in range(1, LEVELS + 1):
            r0, c0, nr, nc = self.keep[-1]
            bit = bit_of(me, order[level])
            if axes[level] == 0:
                nr //= 2
                self.keep.append((pl.multiple_of(r0 + bit * nr, 16), c0, nr, nc))
                self.send.append((pl.multiple_of(r0 + (1 - bit) * nr, 16), c0, nr, nc))
            else:
                nc //= 2
                self.keep.append((r0, pl.multiple_of(c0 + bit * nc, 128), nr, nc))
                self.send.append((r0, pl.multiple_of(c0 + (1 - bit) * nc, 128), nr, nc))

    def half(self, ref, chunk, which):
        size = CHUNK // 2
        start = pl.multiple_of((chunk + self.base) * CHUNK + which * size, size)
        if self.axis_chunk == 0:
            return ref.at[pl.ds(start, size), :]
        return ref.at[:, pl.ds(start, size)]

    @staticmethod
    def at(ref, slot, region):
        r0, c0, nr, nc = region
        return ref.at[slot, pl.ds(r0, nr), pl.ds(c0, nc)]

    def copy(self, phase, chunk):
        me = self.me
        acc_slot, rx_slot, sum_slot = lax.rem(chunk, self.acc_slots), lax.rem(chunk, self.rx_slots), lax.rem(chunk, self.sum_slots)
        core = bit_of(me, CORE)
        if phase == 0:
            source, target = self.half(self.src, chunk, 1 - core), self.rx[0].at[rx_slot]
        elif phase <= LEVELS:
            source, target = self.at(self.acc, acc_slot, self.send[phase]), self.rx[phase].at[rx_slot]
        elif phase <= 2 * LEVELS:
            source = self.at(self.total, sum_slot, self.keep[2 * LEVELS + 1 - phase])
            target = source
        else:
            source, target = self.total.at[sum_slot], self.half(self.out, chunk, core)
        level = phase if phase <= LEVELS else 2 * LEVELS + 1 - phase
        return pltpu.make_async_remote_copy(
            src_ref=source,
            dst_ref=target,
            send_sem=self.send_sem.at[phase, rx_slot],
            recv_sem=self.recv_sem.at[phase, rx_slot],
            device_id=(partner_of(me, self.order[level]),),
            device_id_type=MESH,
        )

    def load(self, chunk):
        slot = lax.rem(chunk, self.acc_slots)
        return pltpu.make_async_copy(self.half(self.src, chunk, bit_of(self.me, CORE)), self.acc.at[slot], self.load_sem.at[slot])

    def store(self, chunk):
        slot = lax.rem(chunk, self.sum_slots)
        return pltpu.make_async_copy(self.total.at[slot], self.half(self.out, chunk, bit_of(self.me, CORE)), self.store_sem.at[slot])

    def add(self, chunk, level, region, parent, target, target_slot):
        acc_slot, rx_slot = lax.rem(chunk, self.acc_slots), lax.rem(chunk, self.rx_slots)
        r0, c0, nr, nc = region
        rel_r, rel_c = r0 - parent[0], c0 - parent[1]
        rows = max(16, min(nr, 24576 // nc))
        rx = self.rx[level]

        def body(i, carry):
            at_r = pl.multiple_of(r0 + i * rows, 16)
            from_r = pl.multiple_of(rel_r + i * rows, 16)
            to_c = c0 if isinstance(c0, int) else pl.multiple_of(c0, 128)
            from_c = rel_c if isinstance(rel_c, int) else pl.multiple_of(rel_c, 128)
            mine = self.acc[acc_slot, pl.ds(at_r, rows), pl.ds(to_c, nc)].astype(jnp.float32)
            theirs = rx[rx_slot, pl.ds(from_r, rows), pl.ds(from_c, nc)].astype(jnp.float32)
            target[target_slot, pl.ds(at_r, rows), pl.ds(to_c, nc)] = (mine + theirs).astype(jnp.bfloat16)
            return carry

        lax.fori_loop(0, nr // rows, body, 0)

    def stage(self, number, chunk):
        if number == 0:
            self.load(chunk).start()
            self.copy(0, chunk).start()
            return
        if number == 1:
            self.load(chunk).wait()
        self.copy(number - 1, chunk).wait()
        if number <= LEVELS:
            slot = lax.rem(chunk, self.acc_slots)
            parent = self.keep[number - 1]
            self.add(chunk, number - 1, self.send[number], parent, self.acc, slot)
            self.copy(number, chunk).start()
            self.add(chunk, number - 1, self.keep[number], parent, self.acc, slot)
        elif number == LEVELS + 1:
            last = self.keep[LEVELS]
            self.add(chunk, LEVELS, last, last, self.total, lax.rem(chunk, self.sum_slots))
            self.copy(number, chunk).start()
        elif number <= 2 * LEVELS:
            self.copy(number, chunk).start()
        elif number == 2 * LEVELS + 1:
            self.copy(number, chunk).start()
            self.store(chunk).start()
        else:
            self.store(chunk).wait()


PART_REFS = 2 + LEVELS + 1 + 4
COL_AXES, ROW_AXES = (1, 0, 0, 0, 0), (0, 0, 0, 0, 1)


def sum_kernel(up_ref, down_ref, head_ref, up_out, down_out, head_out, *scratch):
    me = lax.axis_index('data')
    strides = (CORE, X, Y, Z_LOW, Z_HIGH)
    barrier = pltpu.get_barrier_semaphore()
    for stride in strides:
        pl.semaphore_signal(barrier, inc=1, device_id=(partner_of(me, stride),), device_id_type=MESH)
    pl.semaphore_wait(barrier, len(strides))

    def build(index, src, out, span, first):
        refs = scratch[index * PART_REFS:(index + 1) * PART_REFS]
        acc, rx, total = refs[0], refs[1:2 + LEVELS], refs[2 + LEVELS]
        order = (CORE, X, Z_LOW, Y, Z_HIGH) if index % 2 == 0 else (CORE, Y, Z_LOW, X, Z_HIGH)
        axis_chunk, axes = (0, ROW_AXES) if src is down_ref else (1, COL_AXES)
        return Part(me, axis_chunk, order, axes, src, out, span, first, acc, rx, total, *refs[3 + LEVELS:])

    head_half = head_ref.shape[1] // CHUNK // 2
    parts = (
        build(2, head_ref, head_out, (0, head_half), 0),
        build(3, head_ref, head_out, (head_half, head_half), 0),
        build(0, up_ref, up_out, (0, up_ref.shape[1] // CHUNK), head_half),
        build(1, down_ref, down_out, (0, down_ref.shape[0] // CHUNK), head_half),
    )
    stages = 2 * LEVELS + 3

    def tick(t, carry):
        for number in range(stages):
            for part in parts:
                chunk = t - number - part.first

                @pl.when(jnp.logical_and(chunk >= 0, chunk < part.chunks))
                def _():
                    part.stage(number, chunk)
        return carry

    lax.fori_loop(0, max(part.first + part.chunks for part in parts) + stages - 1, tick, 0)


def part_scratch(rows, cols, axes, slots):
    acc_slots, rx_slots, sum_slots = slots
    shapes = [pltpu.VMEM((acc_slots, rows, cols), jnp.bfloat16), pltpu.VMEM((rx_slots, rows, cols), jnp.bfloat16)]
    nr, nc = rows, cols
    for level in range(1, LEVELS + 1):
        nr, nc = (nr // 2, nc) if axes[level] == 0 else (nr, nc // 2)
        shapes.append(pltpu.VMEM((rx_slots, nr, nc), jnp.bfloat16))
    shapes.append(pltpu.VMEM((sum_slots, rows, cols), jnp.bfloat16))
    phases = 2 * LEVELS + 2
    shapes += [pltpu.SemaphoreType.DMA((phases, rx_slots)), pltpu.SemaphoreType.DMA((phases, rx_slots))]
    shapes += [pltpu.SemaphoreType.DMA((acc_slots,)), pltpu.SemaphoreType.DMA((sum_slots,))]
    return shapes


def sum_gradients(up_local, down_local, head_local):
    slots, head_slots = (ACC_SLOTS, RX_SLOTS, SUM_SLOTS), (head_local.shape[1] // CHUNK // 2,) * 3
    model = up_local.shape[0]
    scratch = part_scratch(model, CHUNK // 2, COL_AXES, slots) + part_scratch(CHUNK // 2, model, ROW_AXES, slots)
    scratch += part_scratch(model, CHUNK // 2, COL_AXES, head_slots) * 2
    any_spec = pl.BlockSpec(memory_space=pl.ANY)
    arrays = (up_local, down_local, head_local)
    size = sum(array.size for array in arrays)
    return pl.pallas_call(
        sum_kernel,
        out_shape=[jax.ShapeDtypeStruct(array.shape, jnp.bfloat16) for array in arrays],
        in_specs=[any_spec] * 3,
        out_specs=[any_spec] * 3,
        scratch_shapes=scratch,
        compiler_params=pltpu.CompilerParams(collective_id=0, has_side_effects=True, vmem_limit_bytes=62 * 2**20),
        cost_estimate=pl.CostEstimate(flops=280 * 10**9, bytes_accessed=8 * size, transcendentals=0),
        name='sum_gradients',
    )(*arrays)


def first_up_kernel(rows_ref, weight_ref, pre_out, act_out):
    pre_act = jnp.dot(rows_ref[...], weight_ref[...].astype(jnp.bfloat16), preferred_element_type=jnp.float32)
    pre_out[...] = pre_act
    act_out[...] = jax.nn.gelu(pre_act).astype(jnp.bfloat16)


def first_down_kernel(rows_ref, act_ref, weight_ref, top_out, hidden):
    step = pl.program_id(0)

    @pl.when(step == 0)
    def _():
        hidden[...] = rows_ref[...].astype(jnp.float32)

    hidden[...] += jnp.dot(act_ref[...], weight_ref[...].astype(jnp.bfloat16), preferred_element_type=jnp.float32)

    @pl.when(step == pl.num_programs(0) - 1)
    def _():
        top_out[...] = hidden[...].astype(jnp.bfloat16)


def first_head_kernel(loss_scale, top_ref, target_ref, weight_ref, share_out, cotangent_out, cotangent):
    step = pl.program_id(0)

    @pl.when(step == 0)
    def _():
        cotangent[...] = jnp.zeros_like(cotangent)

    weight_bf = weight_ref[...].astype(jnp.bfloat16)
    logits = jnp.dot(top_ref[...], weight_bf, preferred_element_type=jnp.float32)
    grad_logits = ((logits - target_ref[...].astype(jnp.float32)) * loss_scale).astype(jnp.bfloat16)
    cotangent[...] += lax.dot_general(grad_logits, weight_bf, COL_DIMS, preferred_element_type=jnp.float32)
    share_out[...] = lax.dot_general(top_ref[...], grad_logits, ROW_DIMS, preferred_element_type=jnp.float32).astype(jnp.bfloat16)

    @pl.when(step == pl.num_programs(0) - 1)
    def _():
        cotangent_out[...] = cotangent[...].astype(jnp.bfloat16)


def update(weight_ref, moment_ref, grad, weight_out, moment_out, rate):
    new_moment = MOMENTUM * moment_ref[...] + grad.astype(jnp.float32)
    new_weight = weight_ref[...] - rate * new_moment
    moment_out[...] = new_moment
    weight_out[...] = new_weight
    return new_weight.astype(jnp.bfloat16)


def up_kernel(rate, rows_ref, weight_ref, moment_ref, grad_ref, weight_out, moment_out, act_out):
    weight_bf = update(weight_ref, moment_ref, grad_ref[...], weight_out, moment_out, rate)
    pre_act = jnp.dot(rows_ref[...], weight_bf, preferred_element_type=jnp.float32)
    act_out[...] = jax.nn.gelu(pre_act).astype(jnp.bfloat16)


def down_kernel(rate, rows_ref, act_ref, weight_ref, moment_ref, grad_ref, weight_out, moment_out, hidden_out, hidden_bf_out):
    step = pl.program_id(0)
    weight_bf = update(weight_ref, moment_ref, grad_ref[...], weight_out, moment_out, rate)

    @pl.when(step == 0)
    def _():
        hidden_out[...] = rows_ref[...].astype(jnp.float32)

    hidden_out[...] += jnp.dot(act_ref[...], weight_bf, preferred_element_type=jnp.float32)

    @pl.when(step == pl.num_programs(0) - 1)
    def _():
        hidden_bf_out[...] = hidden_out[...].astype(jnp.bfloat16)


def head_kernel(rate, hidden_ref, target_ref, weight_ref, moment_ref, grad_ref, weight_out, moment_out, error_out):
    weight_bf = update(weight_ref, moment_ref, grad_ref[...], weight_out, moment_out, rate)
    logits = jnp.dot(hidden_ref[...], weight_bf, preferred_element_type=jnp.float32)
    logit_err = logits - target_ref[...].astype(jnp.float32)
    squares = logit_err * logit_err
    folded = squares[:, :128]
    for start in range(128, squares.shape[1], 128):
        folded += squares[:, start:start + 128]

    @pl.when(pl.program_id(0) == 0)
    def _():
        error_out[...] = jnp.zeros_like(error_out)

    error_out[...] += folded


def whole(shape):
    return pl.BlockSpec(shape, lambda i: (0, 0))


def step_call(kernel, rate, steps, in_specs, out_specs, out_shape, flops, name, args):
    return pl.pallas_call(
        functools.partial(kernel, rate),
        grid=(steps,),
        in_specs=in_specs,
        out_specs=out_specs,
        out_shape=out_shape,
        compiler_params=pltpu.CompilerParams(dimension_semantics=('arbitrary',), vmem_limit_bytes=60 * 2**20),
        cost_estimate=pl.CostEstimate(flops=flops, bytes_accessed=16 * args[-1].size, transcendentals=0),
        name=name,
    )(*args)


def first_call(kernel, steps, in_specs, out_specs, out_shape, scratch, flops, name, args):
    return pl.pallas_call(
        kernel,
        grid=(steps,),
        in_specs=in_specs,
        out_specs=out_specs,
        out_shape=out_shape,
        scratch_shapes=scratch,
        compiler_params=pltpu.CompilerParams(dimension_semantics=('arbitrary',), vmem_limit_bytes=60 * 2**20),
        cost_estimate=pl.CostEstimate(flops=flops, bytes_accessed=4 * args[-1].size, transcendentals=0),
        name=name,
    )(*args)


def first_up(rows, weight, tile=512):
    tokens, (model, width) = rows.shape[0], weight.shape
    cols = pl.BlockSpec((tokens, tile), lambda i: (0, i))
    return first_call(
        first_up_kernel, width // tile, [whole(rows.shape), pl.BlockSpec((model, tile), lambda i: (0, i))], [cols, cols],
        [jax.ShapeDtypeStruct((tokens, width), jnp.float32), jax.ShapeDtypeStruct((tokens, width), jnp.bfloat16)],
        [], 2 * tokens * model * width, 'first_up', (rows, weight))


def first_down(rows, act, weight, tile=512):
    tokens, (width, model) = rows.shape[0], weight.shape
    return first_call(
        first_down_kernel, width // tile,
        [whole(rows.shape), pl.BlockSpec((tokens, tile), lambda i: (0, i)), pl.BlockSpec((tile, model), lambda i: (i, 0))],
        whole(rows.shape), jax.ShapeDtypeStruct(rows.shape, jnp.bfloat16),
        [pltpu.VMEM(rows.shape, jnp.float32)], 2 * tokens * model * width, 'first_down', (rows, act, weight))


def first_head(top_bf, targets, weight, loss_scale, tile=512):
    tokens, (model, width) = top_bf.shape[0], weight.shape
    cols = pl.BlockSpec((model, tile), lambda i: (0, i))
    return first_call(
        functools.partial(first_head_kernel, loss_scale), width // tile,
        [whole(top_bf.shape), pl.BlockSpec((tokens, tile), lambda i: (0, i)), cols],
        [cols, whole(top_bf.shape)], [jax.ShapeDtypeStruct((model, width), jnp.bfloat16), jax.ShapeDtypeStruct(top_bf.shape, jnp.bfloat16)],
        [pltpu.VMEM(top_bf.shape, jnp.float32)], 6 * tokens * model * width, 'first_head', (top_bf, targets, weight))


def second_up(rows, weight, moment, grad, rate, tile=256):
    tokens, (model, width) = rows.shape[0], weight.shape
    cols = pl.BlockSpec((model, tile), lambda i: (0, i))
    return step_call(
        up_kernel, rate, width // tile,
        [whole(rows.shape), cols, cols, cols],
        [cols, cols, pl.BlockSpec((tokens, tile), lambda i: (0, i))],
        [jax.ShapeDtypeStruct(weight.shape, jnp.float32)] * 2 + [jax.ShapeDtypeStruct((tokens, width), jnp.bfloat16)],
        2 * tokens * model * width, 'second_up', (rows, weight, moment, grad))


def second_down(rows, act, weight, moment, grad, rate, tile=384):
    tokens, (width, model) = rows.shape[0], weight.shape
    band = pl.BlockSpec((tile, model), lambda i: (i, 0))
    return step_call(
        down_kernel, rate, width // tile,
        [whole(rows.shape), pl.BlockSpec((tokens, tile), lambda i: (0, i)), band, band, band],
        [band, band, whole(rows.shape), whole(rows.shape)],
        [jax.ShapeDtypeStruct(weight.shape, jnp.float32)] * 2 + [jax.ShapeDtypeStruct(rows.shape, jnp.float32), jax.ShapeDtypeStruct(rows.shape, jnp.bfloat16)],
        2 * tokens * model * width, 'second_down', (rows, act, weight, moment, grad))


def second_head(hidden_bf, targets, weight, moment, grad, rate, tile=256):
    tokens, (model, width) = hidden_bf.shape[0], weight.shape
    cols = pl.BlockSpec((model, tile), lambda i: (0, i))
    return step_call(
        head_kernel, rate, width // tile,
        [whole(hidden_bf.shape), pl.BlockSpec((tokens, tile), lambda i: (0, i)), cols, cols, cols],
        [cols, cols, whole((tokens, 128))],
        [jax.ShapeDtypeStruct(weight.shape, jnp.float32)] * 2 + [jax.ShapeDtypeStruct((tokens, 128), jnp.float32)],
        2 * tokens * model * width, 'second_head', (hidden_bf, targets, weight, moment, grad))


def solution(mesh):
    data_size = mesh.shape['data']

    def device_step(inputs_now, targets_now, inputs_next, targets_next, w_up, w_down, w_head, mom_up, mom_down, mom_head):
        rate = RATE_BASE / w_up.shape[0]
        loss_scale = 1.0 / (inputs_now.shape[0] * data_size * w_head.shape[1])
        up, down, up_moment, down_moment = w_up[0], w_down[0], mom_up[0], mom_down[0]
        down_bf = down.astype(jnp.bfloat16)

        pre_act, act_bf = first_up(inputs_now, up)
        top_bf = first_down(inputs_now, act_bf, down)
        head_local, grad_hidden_bf = first_head(top_bf, targets_now, w_head, loss_scale)
        down_local = lax.dot_general(act_bf, grad_hidden_bf, ROW_DIMS, preferred_element_type=jnp.float32).astype(jnp.bfloat16)
        grad_act = lax.dot_general(grad_hidden_bf, down_bf, COL_DIMS, preferred_element_type=jnp.float32)
        gelu_back = jax.vjp(jax.nn.gelu, pre_act)[1]
        grad_pre = gelu_back(grad_act)[0].astype(jnp.bfloat16)
        up_local = lax.dot_general(inputs_now, grad_pre, ROW_DIMS, preferred_element_type=jnp.float32).astype(jnp.bfloat16)
        grad_up, grad_down, grad_head = sum_gradients(up_local, down_local, head_local)

        up_new, up_moment_new, act_next = second_up(inputs_next, up, up_moment, grad_up, rate)
        down_new, down_moment_new, hidden_next, hidden_next_bf = second_down(inputs_next, act_next, down, down_moment, grad_down, rate)
        head_new, head_moment_new, squares = second_head(hidden_next_bf, targets_next, w_head, mom_head, grad_head, rate)
        errors = jnp.sum(squares, axis=-1) / (2.0 * w_head.shape[1])
        return (up_new[None], down_new[None], head_new, up_moment_new[None], down_moment_new[None], head_moment_new, errors, hidden_next)

    row_spec = P('data', None)
    whole3, whole2 = P(None, None, None), P(None, None)
    in_specs = (row_spec, row_spec, row_spec, row_spec, whole3, whole3, whole2, whole3, whole3, whole2)
    out_specs = (whole3, whole3, whole2, whole3, whole3, whole2, P('data'), row_spec)
    return jax.shard_map(device_step, mesh=mesh, in_specs=in_specs, out_specs=out_specs, check_vma=False)
```
